256 devices in a mesh: grp: 8 (over y, x_lo), seq: 32 (over x_hi, z, core).
Axes of the slice: x: 4 (x_hi: 2, x_lo: 2; x = x_hi * 2 + x_lo), y: 4, z: 8, core: 2. Of those that a mesh axis runs over, the one named last changes fastest.
Arguments:
- queries: bfloat16 [16, 1024, 8192], P('grp', 'seq'), parts along dimension 0, may hold values from -400 to 400
- stretch_keys: bfloat16 [16, 1024, 1024], P('grp', 'seq'), parts along dimension 0, may hold values from -6 to 6
- stretch_values: bfloat16 [16, 1024, 1024], P('grp', 'seq'), parts along dimension 0, may hold values from -6 to 6
- cache_keys: bfloat16 [16, 2048, 1024], P('grp', 'seq'), parts along dimension 0, may hold values from -6 to 6
- cache_values: bfloat16 [16, 2048, 1024], P('grp', 'seq'), parts along dimension 0, may hold values from -6 to 6
- prefix_len: int32 [16], P('grp'), parts along dimension 0, may hold values from 16 to 2048, as said below
Outputs:
- attention: bfloat16 [16, 1024, 8192], P('grp', 'seq'), parts along dimension 0
- prefix_bounds: bfloat16 [16, 128, 2048], P('grp', 'seq'), parts along dimension 0
- stretch_bounds: bfloat16 [16, 64, 2048], P('grp', 'seq'), parts along dimension 0
The draws below stay inside these ranges and needn't reach their ends.
There are 8 independent parts, one for each index of `grp`. The reference program is written for one: setup_inputs(seed, part) draws one part's arguments, and reference() takes and returns one part's arrays. A program takes and returns all parts, laid end to end along the dimension named above; each array names one. Nothing has to cross between parts.
Inputs may be any that keep to these rules, and one draw needn't show every extreme that they name: `prefix_len`: multiples of 16; some sequence of every group has 2048.
All inputs are finite; a program needn't handle non-finite values.
Results may differ from the reference program's by a relative error of at most 0.006.
Values may be sent and summed in bfloat16 or wider, within the bound.
No kernel may reach another device: no remote copies, remote signals or barrier semaphores. Data moves between devices by JAX's collectives and lax.ppermute only.
A program may use at most 128 MiB of HBM per device.

```python
import math
import jax
import jax.numpy as jnp
from jax import lax

HQ = 64
HK = 8
DH = 128
PAGE = 16
SEQS = 2
STRETCH = 1024
PREFIX = 2048


def key_field(base):
    field_values = jnp.clip(jax.random.normal(jax.random.fold_in(base, 11), (SEQS, STRETCH, HK * DH), jnp.float32), -6.0, 6.0)
    return field_values


def draw_stretch_keys(key, part):
    return key_field(key).astype(jnp.bfloat16)


def draw_queries(key, part):
    field_values = jnp.clip(jax.random.normal(jax.random.fold_in(key, 12), (SEQS, STRETCH, HQ * DH), jnp.float32), -6.0, 6.0)
    return field_values.astype(jnp.bfloat16)


def draw_prefix_len(key, part):
    page_count = jax.random.randint(jax.random.fold_in(key, 21), (SEQS,), 1, PREFIX // PAGE + 1)
    full_seq = jax.random.randint(jax.random.fold_in(key, 22), (), 0, SEQS)
    page_count = jnp.where(jnp.arange(SEQS) == full_seq, PREFIX // PAGE, page_count)
    return (page_count * PAGE).astype(jnp.int32)


def steps_of(rng, dims, shards, smallest, high):
    loudness = 1.0
    for dim, blocks in shards:
        steps = jax.random.uniform(jax.random.fold_in(jax.random.fold_in(rng, 6), dim), (blocks,), jnp.float32, smallest / len(shards), high / len(shards))
        loudness = loudness * jnp.repeat(jnp.exp(steps), dims[dim] // blocks).reshape((-1,) + (1,) * (len(dims) - 1 - dim))
    return loudness


def scatter_about(stream_key, extent, spread, most, split=(), kind=jnp.bfloat16):
    factor_of = steps_of(stream_key, extent, split, -0.22, 0.18) if split else 1.0
    array = jax.random.normal(stream_key, extent, jnp.float32) * spread * factor_of
    return jnp.minimum(jnp.maximum(array, -most), most).astype(kind)


def setup_inputs(seed: int = 0, part: int = 0) -> dict:
    keys = jax.random.split(jax.random.key(seed), 7)
    part_splits = jax.random.split(jax.random.fold_in(keys[6], part), 7)
    queries = draw_queries(jax.random.fold_in(jax.random.fold_in(keys[6], part), 71), part)
    stretch_keys = draw_stretch_keys(jax.random.fold_in(jax.random.fold_in(keys[6], part), 71), part)
    stretch_values = scatter_about(part_splits[2], (SEQS, STRETCH, HK * DH), 1.0, 6.0, ((1, 32),))
    cache_keys = scatter_about(part_splits[3], (SEQS, PREFIX, HK * DH), 1.0, 6.0, ((1, 32),))
    cache_values = scatter_about(part_splits[4], (SEQS, PREFIX, HK * DH), 1.0, 6.0, ((1, 32),))
    prefix_len = draw_prefix_len(jax.random.fold_in(jax.random.fold_in(keys[6], part), 71), part)
    return dict(queries=queries, stretch_keys=stretch_keys, stretch_values=stretch_values, cache_keys=cache_keys, cache_values=cache_values, prefix_len=prefix_len)


def page_bounds(key_rows, live_pages):
    shaped = key_rows.reshape(key_rows.shape[0] // PAGE, PAGE, key_rows.shape[1])
    joined = jnp.concatenate([lax.optimization_barrier(jnp.min(shaped, axis=1)), lax.optimization_barrier(jnp.max(shaped, axis=1))], axis=1)
    return jnp.where(live_pages[:, None], joined, jnp.zeros_like(joined))

def reference(queries, stretch_keys, stretch_values, cache_keys, cache_values, prefix_len):
    group = HQ // HK
    factor = 1.0 / math.sqrt(DH)
    block = math.gcd(STRETCH, 256)
    key_index = jnp.arange(PREFIX + STRETCH, dtype=jnp.int32)

    def one_sequence(operands):
        query_rows, new_keys, new_values, old_keys, old_values, length = operands
        key_rows = jnp.concatenate([old_keys, new_keys], axis=0).astype(jnp.float32).reshape(PREFIX + STRETCH, HK, DH)
        value_rows = jnp.concatenate([old_values, new_values], axis=0).astype(jnp.float32).reshape(PREFIX + STRETCH, HK, DH)

        def one_block(offset):
            query_block = lax.dynamic_slice_in_dim(query_rows, offset, block, 0).astype(jnp.float32).reshape(block, HK, group, DH)
            scores = jnp.einsum('rhgd,khd->rhgk', query_block, key_rows) * factor
            row_index = offset + jnp.arange(block, dtype=jnp.int32)
            live = jnp.where(key_index[None, :] < PREFIX, key_index[None, :] < length, key_index[None, :] - PREFIX <= row_index[:, None])
            live = live[:, None, None, :]
            top_score = lax.optimization_barrier(jnp.max(jnp.where(live, scores, -1e+30), axis=-1, keepdims=True))
            weights = jnp.where(live, jnp.exp(scores - top_score), 0.0)
            weight_sum = lax.optimization_barrier(jnp.sum(weights, axis=-1))
            rounded = lax.optimization_barrier(weights.astype(jnp.bfloat16)).astype(jnp.float32)
            mixed = jnp.einsum('rhgk,khd->rhgd', rounded, value_rows) / weight_sum[..., None]
            return mixed.reshape(block, HQ * DH).astype(jnp.bfloat16)
        offsets = jnp.arange(STRETCH // block, dtype=jnp.int32) * block
        attention = lax.map(one_block, offsets).reshape(STRETCH, HQ * DH)
        old_live = jnp.arange(PREFIX // PAGE, dtype=jnp.int32) * PAGE < length
        new_live = jnp.ones((STRETCH // PAGE,), dtype=bool)
        return (attention, page_bounds(old_keys, old_live), page_bounds(new_keys, new_live))
    attention, prefix_bounds, stretch_bounds = lax.map(one_sequence, (queries, stretch_keys, stretch_values, cache_keys, cache_values, prefix_len))
    return (attention, prefix_bounds, stretch_bounds)
```

```python
import functools
import math

import jax
import jax.numpy as jnp
from jax import lax
from jax.experimental import pallas as pl
from jax.experimental.pallas import tpu as pltpu
from jax.sharding import PartitionSpec as P

HQ = 64
HK = 8
DH = 128
PAGE = 16
GROUP = HQ // HK
NEG = -1e30
BIG = 1 << 30
QUAD = 4
RING = 8
KH = HK // QUAD
SCALE = math.log2(math.e) / math.sqrt(DH)


def ring_perm(step):
    return [(i, (i // 16) * 16 + ((i // 2 + step) % RING) * 2 + i % 2) for i in range(32)]


def quad_perm(r):
    return [(i, i ^ ((r >> 1) * 16) ^ (r & 1)) for i in range(32)]


def pack_kv(place, cache_keys, cache_values, stretch_keys, stretch_values):
    seqs, pre, _ = cache_keys.shape
    new = stretch_keys.shape[1]

    def body(place_ref, ck, cv, sk, sv, *outs):
        own = place_ref[0]
        for s in range(seqs):
            for r in range(QUAD):
                for h in range(KH):
                    at = pl.ds(pl.multiple_of((own ^ r) * (KH * DH) + h * DH, DH), DH)
                    out = outs[s * QUAD + r]
                    for kv, (old, fresh) in enumerate(((ck, sk), (cv, sv))):
                        out[kv, h, :pre, :] = old[s, :, at]
                        out[kv, h, pre:, :] = fresh[s, :, at]

    shape = jax.ShapeDtypeStruct((2, KH, pre + new, DH), jnp.bfloat16)
    outs = pl.pallas_call(
        body,
        in_specs=[pl.BlockSpec(memory_space=pltpu.SMEM)] + [pl.BlockSpec(memory_space=pltpu.VMEM)] * 4,
        out_specs=[pl.BlockSpec(memory_space=pltpu.VMEM)] * (seqs * QUAD),
        out_shape=[shape] * (seqs * QUAD),
        name="pack_kv",
    )(place, cache_keys, cache_values, stretch_keys, stretch_values)
    return [outs[s * QUAD : (s + 1) * QUAD] for s in range(seqs)]


def pack_q(place, queries):
    seqs, rows, _ = queries.shape

    def body(place_ref, q, *outs):
        own = place_ref[0]
        for r in range(QUAD):
            for h in range(KH):
                for g in range(GROUP):
                    at = (own ^ r) * (KH * GROUP * DH) + (h * GROUP + g) * DH
                    outs[r][0, h, g * rows : (g + 1) * rows, :] = q[0, :, pl.ds(pl.multiple_of(at, DH), DH)]

    block = (1, KH, GROUP * rows, DH)
    return pl.pallas_call(
        body,
        grid=(seqs,),
        in_specs=[pl.BlockSpec(memory_space=pltpu.SMEM), pl.BlockSpec((1, rows, HQ * DH), lambda s: (s, 0, 0))],
        out_specs=[pl.BlockSpec(block, lambda s: (s, 0, 0, 0))] * QUAD,
        out_shape=[jax.ShapeDtypeStruct((seqs,) + block[1:], jnp.bfloat16)] * QUAD,
        name="pack_q",
    )(place, queries)


def unpack_out(place, pieces, rows):
    seqs = len(pieces)

    def body(place_ref, *refs):
        own = place_ref[0]
        out = refs[-1]
        for s in range(seqs):
            for r in range(QUAD):
                for h in range(KH):
                    for g in range(GROUP):
                        at = (own ^ r) * (KH * GROUP * DH) + (h * GROUP + g) * DH
                        piece = refs[s * QUAD + r][h, g * rows : (g + 1) * rows, :]
                        out[s, :, pl.ds(pl.multiple_of(at, DH), DH)] = piece

    return pl.pallas_call(
        body,
        in_specs=[pl.BlockSpec(memory_space=pltpu.SMEM)] + [pl.BlockSpec(memory_space=pltpu.VMEM)] * (seqs * QUAD),
        out_specs=pl.BlockSpec(memory_space=pltpu.VMEM),
        out_shape=jax.ShapeDtypeStruct((seqs, rows, HQ * DH), jnp.bfloat16),
        name="unpack_out",
    )(place, *[p for one in pieces for p in one])


def bounds(place, prefix_len, cache_keys, stretch_keys):
    seqs, pre, width = cache_keys.shape
    new = stretch_keys.shape[1]

    def body(place_ref, len_ref, ck, sk, pre_out, new_out):
        first = place_ref[1] * (pre // PAGE)
        for s in range(seqs):
            for p in range(pre // PAGE):
                rows = ck[s, p * PAGE : (p + 1) * PAGE, :].astype(jnp.float32)
                live = (first + p) * PAGE < len_ref[s]
                low = jnp.where(live, jnp.min(rows, axis=0, keepdims=True), 0.0)
                high = jnp.where(live, jnp.max(rows, axis=0, keepdims=True), 0.0)
                pre_out[s, p : p + 1, :width] = low.astype(jnp.bfloat16)
                pre_out[s, p : p + 1, width:] = high.astype(jnp.bfloat16)
            for p in range(new // PAGE):
                rows = sk[s, p * PAGE : (p + 1) * PAGE, :].astype(jnp.float32)
                new_out[s, p : p + 1, :width] = jnp.min(rows, axis=0, keepdims=True).astype(jnp.bfloat16)
                new_out[s, p : p + 1, width:] = jnp.max(rows, axis=0, keepdims=True).astype(jnp.bfloat16)

    return pl.pallas_call(
        body,
        in_specs=[pl.BlockSpec(memory_space=pltpu.SMEM)] * 2 + [pl.BlockSpec(memory_space=pltpu.VMEM)] * 2,
        out_specs=[pl.BlockSpec(memory_space=pltpu.VMEM)] * 2,
        out_shape=[
            jax.ShapeDtypeStruct((seqs, pre // PAGE, 2 * width), jnp.bfloat16),
            jax.ShapeDtypeStruct((seqs, new // PAGE, 2 * width), jnp.bfloat16),
        ],
        name="page_bounds",
    )(place, prefix_len, cache_keys, stretch_keys)


def attend(s, bases, queries, blocks, which, key_limit, state, last, rows):
    count = len(blocks)
    tile = GROUP * rows
    length = blocks[0].shape[1] * blocks[0].shape[3]

    def body(*refs):
        base_ref, limit_ref = refs[:2]
        q_refs = refs[2 : 2 + QUAD]
        kv_refs = refs[2 + QUAD : 2 + QUAD + count]
        rest = refs[2 + QUAD + count :]
        if state is not None:
            acc_in, ml_in = rest[:2]
            rest = rest[2:]
        keys = [ref[0, :, 0].reshape(length, DH) for ref in kv_refs]
        values = [ref[1, :, 0].reshape(length, DH) for ref in kv_refs]
        for r in range(QUAD):
            q = q_refs[r][0, 0]
            at = slice(r * tile, (r + 1) * tile)
            row_pos = base_ref[r] + (lax.broadcasted_iota(jnp.int32, (tile, 1), 0) % rows)
            scores = []
            for key, d in zip(keys, which):
                part = lax.dot_general(q, key, (((1,), (1,)), ((), ())), preferred_element_type=jnp.float32)
                scores.append(jnp.where(limit_ref[0, d : d + 1, :] <= row_pos, part, NEG))
            top = jnp.max(functools.reduce(jnp.maximum, scores), axis=-1, keepdims=True)
            if state is not None:
                old_top = ml_in[0, at, 0:1]
                top = jnp.maximum(top, old_top)
            total, mixed = 0.0, 0.0
            for part, value in zip(scores, values):
                weights = jnp.exp2((part - top) * SCALE)
                total = total + weights
                mixed = mixed + jnp.dot(
                    weights.astype(jnp.bfloat16), value, preferred_element_type=jnp.float32
                )
            total = jnp.sum(total, axis=-1, keepdims=True)
            if state is not None:
                shrink = jnp.exp2((old_top - top) * SCALE)
                total = total + ml_in[0, at, DH // 2 : DH // 2 + 1] * shrink
                mixed = mixed + acc_in[0, at, :] * shrink
            if last:
                rest[r][0] = (mixed / total).astype(jnp.bfloat16)
            else:
                rest[0][0, at, :] = mixed
                lane = lax.broadcasted_iota(jnp.int32, (tile, DH), 1)
                rest[1][0, at, :] = jnp.where(lane < DH // 2, top, total)

    state_spec = pl.BlockSpec((1, QUAD * tile, DH), lambda h: (h, 0, 0))
    in_specs = [
        pl.BlockSpec(memory_space=pltpu.SMEM),
        pl.BlockSpec((1,) + key_limit.shape[1:], lambda h: (s, 0, 0)),
    ]
    in_specs += [pl.BlockSpec((1, 1, tile, DH), lambda h: (s, h, 0, 0))] * QUAD
    in_specs += [pl.BlockSpec((2, QUAD, 1) + blocks[0].shape[3:], lambda h: (0, 0, h, 0, 0))] * count
    operands = [bases, key_limit, *queries, *blocks]
    if state is not None:
        in_specs += [state_spec] * 2
        operands += list(state)
    if last:
        out_specs = [pl.BlockSpec((1, tile, DH), lambda h: (h, 0, 0))] * QUAD
        out_shape = [jax.ShapeDtypeStruct((KH, tile, DH), jnp.bfloat16)] * QUAD
    else:
        out_specs = [state_spec] * 2
        out_shape = [jax.ShapeDtypeStruct((KH, QUAD * tile, DH), jnp.float32)] * 2
    pairs = KH * QUAD * tile * length * count
    return pl.pallas_call(
        body,
        grid=(KH,),
        in_specs=in_specs,
        out_specs=out_specs,
        out_shape=out_shape,
        cost_estimate=pl.CostEstimate(flops=4 * DH * pairs, transcendentals=pairs, bytes_accessed=4 << 20),
        name="attend",
    )(*operands)


def on_device(queries, stretch_keys, stretch_values, cache_keys, cache_values, prefix_len):
    seqs, rows, _ = queries.shape
    pre = cache_keys.shape[1]
    index = lax.axis_index("seq").astype(jnp.int32)
    own = (index // 16) * 2 + index % 2
    z = (index // 2) % RING
    place = jnp.stack([own, index])

    pieces = pack_kv(place, cache_keys, cache_values, stretch_keys, stretch_values)
    mine = []
    for s in range(seqs):
        got = [pieces[s][0]] + [lax.ppermute(pieces[s][r], "seq", quad_perm(r)) for r in range(1, QUAD)]
        mine.append(jnp.stack(got, axis=1))
    packed = pack_q(place, queries)
    q_tiles = [packed[0]] + [lax.ppermute(packed[r], "seq", quad_perm(r)) for r in range(1, QUAD)]
    prefix_bounds, stretch_bounds = bounds(place, prefix_len, cache_keys, stretch_keys)

    peer = own ^ jnp.arange(QUAD, dtype=jnp.int32)
    plane = (z + jnp.arange(RING, dtype=jnp.int32)) % RING
    shard = (peer // 2 * 16 + peer % 2)[None, :] + plane[:, None] * 2
    old_pos = shard[:, :, None] * pre + jnp.arange(pre, dtype=jnp.int32)
    new_pos = shard[:, :, None] * rows + jnp.arange(rows, dtype=jnp.int32)
    old_limit = jnp.where(old_pos[None] < prefix_len[:, None, None, None], -1, BIG)
    new_limit = jnp.broadcast_to(new_pos[None], (seqs,) + new_pos.shape)
    key_limit = jnp.concatenate([old_limit, new_limit], axis=3).reshape(seqs, RING, -1)
    bases = shard[0] * rows

    blocks = []
    for s in range(seqs):
        forth, back = [mine[s]], [mine[s]]
        blocks.append({0: mine[s]})
    for step in range(1, RING // 2 + 1):
        for s in range(seqs):
            if step < RING // 2 or s % 2 == 0:
                blocks[s][-step % RING] = lax.ppermute(blocks[s][(1 - step) % RING], "seq", ring_perm(1))
            if step < RING // 2 or s % 2 == 1:
                blocks[s][step % RING] = lax.ppermute(blocks[s][(step - 1) % RING], "seq", ring_perm(-1))

    sent = []
    for s in range(seqs):
        state = None
        for which in ((0, 7, 1), (6, 2), (5, 3), (4,)):
            state = attend(
                s, bases, q_tiles, [blocks[s][d] for d in which], which, key_limit, state, which[0] == 4, rows
            )
        sent.append([state[0]] + [lax.ppermute(state[r], "seq", quad_perm(r)) for r in range(1, QUAD)])
    attention = unpack_out(place, sent, rows)
    return attention, prefix_bounds, stretch_bounds


def solution(mesh):
    return jax.shard_map(
        on_device,
        mesh=mesh,
        in_specs=(
            P("grp", "seq", None),
            P("grp", "seq", None),
            P("grp", "seq", None),
            P("grp", "seq", None),
            P("grp", "seq", None),
            P("grp"),
        ),
        out_specs=(P("grp", "seq", None), P("grp", "seq", None), P("grp", "seq", None)),
        check_vma=False,
    )
```

```python
import math

import jax
import jax.numpy as jnp
from jax import lax
from jax.experimental import pallas as pl
from jax.experimental.pallas import tpu as pltpu
from jax.sharding import PartitionSpec as P

HQ = 64
HK = 8
DH = 128
PAGE = 16
GROUP = HQ // HK
NEG = -1e30
QUAD = 4
RING = 8
KH = HK // QUAD
PHASES = ((0, 7, 1, 6, 2), (5, 3, 4))
SCALE = math.log2(math.e) / math.sqrt(DH)


def ring_perm(step):
    return [(i, (i // 16) * 16 + ((i // 2 + step) % RING) * 2 + i % 2) for i in range(32)]


def quad_perm(r):
    return [(i, i ^ ((r >> 1) * 16) ^ (r & 1)) for i in range(32)]


def corner(place_ref):
    return (place_ref[0] // 16) * 2 + place_ref[0] % 2


def pack_kv(s, place, cache_keys, cache_values, stretch_keys, stretch_values):
    pre, new = cache_keys.shape[1], stretch_keys.shape[1]

    def body(place_ref, ck, cv, sk, sv, *outs):
        own = corner(place_ref)
        for r in range(QUAD):
            for h in range(KH):
                at = pl.ds(pl.multiple_of((own ^ r) * (KH * DH) + h * DH, DH), DH)
                for kv, (old, fresh) in enumerate(((ck, sk), (cv, sv))):
                    outs[r][kv, h, :pre, :] = old[0, :, at]
                    outs[r][kv, h, pre:, :] = fresh[0, :, at]

    shape = (2, KH, pre + new, DH)
    spec = lambda x: pl.BlockSpec((1,) + x.shape[1:], lambda i: (s, 0, 0))
    arrays = (cache_keys, cache_values, stretch_keys, stretch_values)
    return pl.pallas_call(
        body,
        grid=(1,),
        in_specs=[pl.BlockSpec(memory_space=pltpu.SMEM)] + [spec(x) for x in arrays],
        out_specs=[pl.BlockSpec(shape, lambda i: (0, 0, 0, 0))] * QUAD,
        out_shape=[jax.ShapeDtypeStruct(shape, jnp.bfloat16)] * QUAD,
        name="pack_kv",
    )(place, *arrays)


def pack_q(place, queries):
    seqs, rows, _ = queries.shape

    def body(place_ref, q, *outs):
        own = corner(place_ref)
        for r in range(QUAD):
            for h in range(KH):
                for g in range(GROUP):
                    at = (own ^ r) * (KH * GROUP * DH) + (h * GROUP + g) * DH
                    outs[r][0, h, g * rows : (g + 1) * rows, :] = q[0, :, pl.ds(pl.multiple_of(at, DH), DH)]

    block = (1, KH, GROUP * rows, DH)
    return pl.pallas_call(
        body,
        grid=(seqs,),
        in_specs=[pl.BlockSpec(memory_space=pltpu.SMEM), pl.BlockSpec((1, rows, HQ * DH), lambda s: (s, 0, 0))],
        out_specs=[pl.BlockSpec(block, lambda s: (s, 0, 0, 0))] * QUAD,
        out_shape=[jax.ShapeDtypeStruct((seqs,) + block[1:], jnp.bfloat16)] * QUAD,
        name="pack_q",
    )(place, queries)


def unpack_out(place, pieces, rows):
    seqs = len(pieces)

    def body(place_ref, *refs):
        own = corner(place_ref)
        out = refs[-1]
        for s in range(seqs):
            for r in range(QUAD):
                for h in range(KH):
                    for g in range(GROUP):
                        at = (own ^ r) * (KH * GROUP * DH) + (h * GROUP + g) * DH
                        piece = refs[s * QUAD + r][h, g * rows : (g + 1) * rows, :]
                        out[s, :, pl.ds(pl.multiple_of(at, DH), DH)] = piece

    return pl.pallas_call(
        body,
        in_specs=[pl.BlockSpec(memory_space=pltpu.SMEM)] + [pl.BlockSpec(memory_space=pltpu.VMEM)] * (seqs * QUAD),
        out_specs=pl.BlockSpec(memory_space=pltpu.VMEM),
        out_shape=jax.ShapeDtypeStruct((seqs, rows, HQ * DH), jnp.bfloat16),
        name="unpack_out",
    )(place, *[p for one in pieces for p in one])


def bounds(place, prefix_len, cache_keys, stretch_keys):
    seqs, pre, width = cache_keys.shape
    new = stretch_keys.shape[1]

    def body(place_ref, len_ref, ck, sk, pre_out, new_out):
        first = place_ref[0] * (pre // PAGE)
        for s in range(seqs):
            for p in range(pre // PAGE):
                rows = ck[s, p * PAGE : (p + 1) * PAGE, :].astype(jnp.float32)
                live = (first + p) * PAGE < len_ref[s]
                low = jnp.where(live, jnp.min(rows, axis=0, keepdims=True), 0.0)
                high = jnp.where(live, jnp.max(rows, axis=0, keepdims=True), 0.0)
                pre_out[s, p : p + 1, :width] = low.astype(jnp.bfloat16)
                pre_out[s, p : p + 1, width:] = high.astype(jnp.bfloat16)
            for p in range(new // PAGE):
                rows = sk[s, p * PAGE : (p + 1) * PAGE, :].astype(jnp.float32)
                new_out[s, p : p + 1, :width] = jnp.min(rows, axis=0, keepdims=True).astype(jnp.bfloat16)
                new_out[s, p : p + 1, width:] = jnp.max(rows, axis=0, keepdims=True).astype(jnp.bfloat16)

    return pl.pallas_call(
        body,
        in_specs=[pl.BlockSpec(memory_space=pltpu.SMEM)] * 2 + [pl.BlockSpec(memory_space=pltpu.VMEM)] * 2,
        out_specs=[pl.BlockSpec(memory_space=pltpu.VMEM)] * 2,
        out_shape=[
            jax.ShapeDtypeStruct((seqs, pre // PAGE, 2 * width), jnp.bfloat16),
            jax.ShapeDtypeStruct((seqs, new // PAGE, 2 * width), jnp.bfloat16),
        ],
        name="page_bounds",
    )(place, prefix_len, cache_keys, stretch_keys)


def attend(s, place, prefix_len, queries, blocks, which, state, last, rows):
    count = len(blocks)
    tile = GROUP * rows
    pre = blocks[0][0].shape[3] - rows
    old_chunks = QUAD * pre // DH
    chunks = old_chunks + QUAD * rows // DH

    def body(*refs):
        place_ref, len_ref = refs[:2]
        q_refs = refs[2 : 2 + QUAD]
        k_refs = refs[2 + QUAD : 2 + QUAD + count]
        v_refs = refs[2 + QUAD + count : 2 + QUAD + 2 * count]
        rest = refs[2 + QUAD + 2 * count : -1]
        score_ref = refs[-1]
        if state is not None:
            mixed_in, top_in = rest[:2]
            rest = rest[2:]
        own = corner(place_ref)
        z = (place_ref[0] // 2) % RING
        lane = lax.broadcasted_iota(jnp.int32, (1, DH), 1)

        def shard(slot, d):
            peer = own ^ slot
            return (peer // 2) * 16 + peer % 2 + ((z + d) % RING) * 2

        def spread(first, width, d):
            pos = shard(first, d) * width + lane
            for k in range(1, DH // width):
                pos = jnp.where(lane >= k * width, shard(first + k, d) * width + lane - k * width, pos)
            return pos

        per = DH // pre
        fade = [
            [jnp.where(spread(c * per, pre, d) < len_ref[s], 0.0, NEG) for c in range(old_chunks)] for d in which
        ]
        new_pos = [spread(0, rows, d) for d in which]
        ones = jnp.ones((QUAD * (pre + rows), DH), jnp.bfloat16)

        def side(ref):
            old = ref[0, :, 0, :pre, :].reshape(QUAD * pre, DH)
            return jnp.concatenate([old, ref[0, :, 0, pre:, :].reshape(QUAD * rows, DH)], axis=0)

        def score(r):
            q = q_refs[r][0, 0]
            row_pos = shard(r, 0) * rows + lax.broadcasted_iota(jnp.int32, (tile, DH), 0) % rows
            top = None
            for b in range(count):
                part = lax.dot_general(
                    q, side(k_refs[b]), (((1,), (1,)), ((), ())), preferred_element_type=jnp.float32
                )
                for c in range(chunks):
                    piece = part[:, c * DH : (c + 1) * DH]
                    if c < old_chunks:
                        piece = piece + fade[b][c]
                    else:
                        piece = jnp.where(new_pos[b] <= row_pos, piece, NEG)
                    score_ref[r % 2, b * chunks + c] = piece
                    top = piece if top is None else jnp.maximum(top, piece)
            return top

        def mix(r, top):
            at = slice(r * tile, (r + 1) * tile)
            top = jnp.broadcast_to(jnp.max(top, axis=-1, keepdims=True), (tile, DH))
            if state is not None:
                old_top = top_in[0, at, :]
                top = jnp.maximum(top, old_top)
            mixed = None
            for b in range(count):
                weights = [
                    jnp.exp2((score_ref[r % 2, b * chunks + c] - top) * SCALE).astype(jnp.bfloat16)
                    for c in range(chunks)
                ]
                part = jnp.dot(
                    jnp.concatenate(weights, axis=1),
                    jnp.concatenate([side(v_refs[b]), ones], axis=1),
                    preferred_element_type=jnp.float32,
                )
                mixed = part if mixed is None else mixed + part
            total, mixed = mixed[:, DH:], mixed[:, :DH]
            if state is not None:
                shrink = jnp.exp2((old_top - top) * SCALE)
                mixed = mixed + mixed_in[0, at, :DH] * shrink
                total = total + mixed_in[0, at, DH:] * shrink
            if last:
                rest[r][0] = (mixed / total).astype(jnp.bfloat16)
            else:
                rest[0][0, at, :DH] = mixed
                rest[0][0, at, DH:] = total
                rest[1][0, at, :] = top

        tops = score(0)
        for r in range(QUAD):
            following = score(r + 1) if r + 1 < QUAD else None
            mix(r, tops)
            tops = following

    kv_shape = (1, QUAD, 1) + blocks[0][0].shape[3:]
    kv_spec = lambda x, i: pl.BlockSpec(kv_shape, lambda h: (min(i, x.shape[0] - 1), 0, h, 0, 0))
    state_specs = [
        pl.BlockSpec((1, QUAD * tile, 2 * DH), lambda h: (h, 0, 0)),
        pl.BlockSpec((1, QUAD * tile, DH), lambda h: (h, 0, 0)),
    ]
    in_specs = [pl.BlockSpec(memory_space=pltpu.SMEM)] * 2
    in_specs += [pl.BlockSpec((1, 1, tile, DH), lambda h: (s, h, 0, 0))] * QUAD
    in_specs += [kv_spec(k, 0) for k, _ in blocks] + [kv_spec(v, 1) for _, v in blocks]
    operands = [place, prefix_len, *queries, *[k for k, _ in blocks], *[v for _, v in blocks]]
    if state is not None:
        in_specs += state_specs
        operands += list(state)
    if last:
        out_specs = [pl.BlockSpec((1, tile, DH), lambda h: (h, 0, 0))] * QUAD
        out_shape = [jax.ShapeDtypeStruct((KH, tile, DH), jnp.bfloat16)] * QUAD
    else:
        out_specs = state_specs
        out_shape = [jax.ShapeDtypeStruct((KH, QUAD * tile, w), jnp.float32) for w in (2 * DH, DH)]
    pairs = KH * QUAD * tile * chunks * DH * count
    return pl.pallas_call(
        body,
        grid=(KH,),
        in_specs=in_specs,
        out_specs=out_specs,
        out_shape=out_shape,
        scratch_shapes=[pltpu.VMEM((2, count * chunks, tile, DH), jnp.float32)],
        cost_estimate=pl.CostEstimate(flops=4 * DH * pairs, transcendentals=pairs, bytes_accessed=4 << 20),
        name="attend",
    )(*operands)


def send(array, perm):
    return lax.ppermute(array, "seq", perm)


def run(queries, stretch_keys, stretch_values, cache_keys, cache_values, prefix_len):
    seqs, rows, _ = queries.shape
    place = lax.axis_index("seq").astype(jnp.int32).reshape(1)

    mine = []
    for s in range(seqs):
        pieces = pack_kv(s, place, cache_keys, cache_values, stretch_keys, stretch_values)
        got = [pieces[0]] + [send(pieces[r], quad_perm(r)) for r in range(1, QUAD)]
        mine.append(jnp.stack(got, axis=1))
    packed = pack_q(place, queries)
    q_tiles = [packed[0]] + [send(packed[r], quad_perm(r)) for r in range(1, QUAD)]
    prefix_bounds, stretch_bounds = bounds(place, prefix_len, cache_keys, stretch_keys)

    blocks = [{0: (m, m)} for m in mine]
    half = RING // 2
    for step in range(1, half):
        for s in range(seqs):
            forth = send(blocks[s][(1 - step) % RING][0], ring_perm(1))
            back = send(blocks[s][step - 1][0], ring_perm(-1))
            blocks[s][-step % RING] = (forth, forth)
            blocks[s][step] = (back, back)
    for s in range(seqs):
        forth = send(blocks[s][half + 1][0][:1], ring_perm(1))
        back = send(blocks[s][half - 1][1][1:], ring_perm(-1))
        blocks[s][half] = (forth, back)

    sent = []
    for s in range(seqs):
        state = None
        for n, which in enumerate(PHASES):
            last = n + 1 == len(PHASES)
            state = attend(
                s, place, prefix_len, q_tiles, [blocks[s][d] for d in which], which, state, last, rows
            )
        sent.append([state[0]] + [send(state[r], quad_perm(r)) for r in range(1, QUAD)])
    attention = unpack_out(place, sent, rows)
    return attention, prefix_bounds, stretch_bounds


def solution(mesh):
    return jax.shard_map(
        run,
        mesh=mesh,
        in_specs=(
            P("grp", "seq", None),
            P("grp", "seq", None),
            P("grp", "seq", None),
            P("grp", "seq", None),
            P("grp", "seq", None),
            P("grp"),
        ),
        out_specs=(P("grp", "seq", None), P("grp", "seq", None), P("grp", "seq", None)),
        check_vma=False,
    )
```

```python
import math

import jax
import jax.numpy as jnp
from jax import lax
from jax.experimental import pallas as pl
from jax.experimental.pallas import tpu as pltpu
from jax.sharding import PartitionSpec as P


HQ = 64
HK = 8
DH = 128
PAGE = 16
GROUP = HQ // HK
NEG = -1e30
QUAD = 4
RING = 8
KH = HK // QUAD
PHASES = ((0, 7, 1), (6, 2), (5, 3), (4,))
ATTEND_VMEM = 24 << 20
SMALL_VMEM = 8 << 20
SCALE = math.log2(math.e) / math.sqrt(DH)


def ring_perm(step):
    return [(i, (i // 16) * 16 + ((i // 2 + step) % RING) * 2 + i % 2) for i in range(32)]


def quad_perm(r):
    return [(i, i ^ ((r >> 1) * 16) ^ (r & 1)) for i in range(32)]


def corner(place_ref):
    return (place_ref[0] // 16) * 2 + place_ref[0] % 2


def pack_kv(place, cache_keys, cache_values, stretch_keys, stretch_values):
    seqs, pre, _ = cache_keys.shape
    new = stretch_keys.shape[1]

    def body(place_ref, ck, cv, sk, sv, *outs):
        own = corner(place_ref)
        for r in range(QUAD):
            for h in range(KH):
                at = pl.ds(pl.multiple_of((own ^ r) * (KH * DH) + h * DH, DH), DH)
                for kv, (old, fresh) in enumerate(((ck, sk), (cv, sv))):
                    for s in range(seqs):
                        outs[r][kv, s, h, :pre, :] = old[s, :, at]
                        outs[r][kv, s, h, pre:, :] = fresh[s, :, at]

    shape = jax.ShapeDtypeStruct((2, seqs, KH, pre + new, DH), jnp.bfloat16)
    return pl.pallas_call(
        body,
        in_specs=[pl.BlockSpec(memory_space=pltpu.SMEM)] + [pl.BlockSpec(memory_space=pltpu.VMEM)] * 4,
        out_specs=[pl.BlockSpec(memory_space=pltpu.VMEM)] * QUAD,
        out_shape=[shape] * QUAD,
        compiler_params=pltpu.CompilerParams(vmem_limit_bytes=SMALL_VMEM),
        name="pack_kv",
    )(place, *[pltpu.with_memory_space_constraint(x, pltpu.HBM) for x in (cache_keys, cache_values, stretch_keys, stretch_values)])


def pack_q(place, queries):
    seqs, rows, _ = queries.shape

    def body(place_ref, q, *outs):
        own = corner(place_ref)
        for r in range(QUAD):
            for h in range(KH):
                for g in range(GROUP):
                    at = (own ^ r) * (KH * GROUP * DH) + (h * GROUP + g) * DH
                    outs[r][0, h, g * rows : (g + 1) * rows, :] = q[0, :, pl.ds(pl.multiple_of(at, DH), DH)]

    block = (1, KH, GROUP * rows, DH)
    return pl.pallas_call(
        body,
        grid=(seqs,),
        in_specs=[pl.BlockSpec(memory_space=pltpu.SMEM), pl.BlockSpec((1, rows, HQ * DH), lambda s: (s, 0, 0))],
        out_specs=[pl.BlockSpec(block, lambda s: (s, 0, 0, 0))] * QUAD,
        out_shape=[jax.ShapeDtypeStruct((seqs,) + block[1:], jnp.bfloat16)] * QUAD,
        compiler_params=pltpu.CompilerParams(vmem_limit_bytes=SMALL_VMEM),
        name="pack_q",
    )(place, queries)


def unpack_out(place, pieces, rows):
    seqs = len(pieces)

    def body(place_ref, *refs):
        own = corner(place_ref)
        out = refs[-1]
        for s in range(seqs):
            for r in range(QUAD):
                for h in range(KH):
                    for g in range(GROUP):
                        at = (own ^ r) * (KH * GROUP * DH) + (h * GROUP + g) * DH
                        piece = refs[s * QUAD + r][h, g * rows : (g + 1) * rows, :]
                        out[s, :, pl.ds(pl.multiple_of(at, DH), DH)] = piece

    return pl.pallas_call(
        body,
        in_specs=[pl.BlockSpec(memory_space=pltpu.SMEM)] + [pl.BlockSpec(memory_space=pltpu.VMEM)] * (seqs * QUAD),
        out_specs=pl.BlockSpec(memory_space=pltpu.VMEM),
        out_shape=jax.ShapeDtypeStruct((seqs, rows, HQ * DH), jnp.bfloat16),
        compiler_params=pltpu.CompilerParams(vmem_limit_bytes=SMALL_VMEM),
        name="unpack_out",
    )(place, *[p for one in pieces for p in one])


def bounds(place, prefix_len, cache_keys, stretch_keys):
    seqs, pre, width = cache_keys.shape
    new = stretch_keys.shape[1]

    def body(place_ref, len_ref, ck, sk, pre_out, new_out):
        first = place_ref[0] * (pre // PAGE)
        for s in range(seqs):
            for p in range(pre // PAGE):
                rows = ck[s, p * PAGE : (p + 1) * PAGE, :].astype(jnp.float32)
                live = (first + p) * PAGE < len_ref[s]
                low = jnp.where(live, jnp.min(rows, axis=0, keepdims=True), 0.0)
                high = jnp.where(live, jnp.max(rows, axis=0, keepdims=True), 0.0)
                pre_out[s, p : p + 1, :width] = low.astype(jnp.bfloat16)
                pre_out[s, p : p + 1, width:] = high.astype(jnp.bfloat16)
            for p in range(new // PAGE):
                rows = sk[s, p * PAGE : (p + 1) * PAGE, :].astype(jnp.float32)
                new_out[s, p : p + 1, :width] = jnp.min(rows, axis=0, keepdims=True).astype(jnp.bfloat16)
                new_out[s, p : p + 1, width:] = jnp.max(rows, axis=0, keepdims=True).astype(jnp.bfloat16)

    return pl.pallas_call(
        body,
        in_specs=[pl.BlockSpec(memory_space=pltpu.SMEM)] * 2 + [pl.BlockSpec(memory_space=pltpu.VMEM)] * 2,
        out_specs=[pl.BlockSpec(memory_space=pltpu.VMEM)] * 2,
        out_shape=[
            jax.ShapeDtypeStruct((seqs, pre // PAGE, 2 * width), jnp.bfloat16),
            jax.ShapeDtypeStruct((seqs, new // PAGE, 2 * width), jnp.bfloat16),
        ],
        compiler_params=pltpu.CompilerParams(vmem_limit_bytes=SMALL_VMEM),
        name="page_bounds",
    )(place, prefix_len, cache_keys, stretch_keys)


def attend(s, place, prefix_len, queries, blocks, which, state, last, rows):
    count = len(blocks)
    tile = GROUP * rows
    slots = QUAD // 2
    pre = blocks[0][0].shape[4] - rows
    half_rows = slots * rows

    def body(*refs):
        place_ref, len_ref = refs[:2]
        q_refs = refs[2 : 2 + QUAD]
        half_refs = refs[2 + QUAD : 2 + QUAD + 2 * count]
        rest = refs[2 + QUAD + 2 * count : -1]
        score_ref = refs[-1]
        if state is not None:
            mixed_in, top_in = rest[:2]
            rest = rest[2:]
        own = corner(place_ref)
        z = (place_ref[0] // 2) % RING
        lane = lax.broadcasted_iota(jnp.int32, (1, DH), 1)

        def shard(slot, d):
            peer = own ^ slot
            return (peer // 2) * 16 + peer % 2 + ((z + d) % RING) * 2

        def spread(first, width, d):
            pos = shard(first, d) * width + lane
            for k in range(1, DH // width):
                pos = jnp.where(lane >= k * width, shard(first + k, d) * width + lane - k * width, pos)
            return pos

        def old_part(ref, kv):
            return ref[:, kv, 0, 0, :pre, :].reshape(slots * pre, DH)

        def new_part(ref, kv):
            return ref[:, kv, 0, 0, pre:, :].reshape(half_rows, DH)

        chunks = []
        for b, d in enumerate(which):
            for half in range(2):
                ref = half_refs[2 * b + half]
                fade = jnp.where(spread(half * slots, pre, d) < len_ref[s], 0.0, NEG)
                chunks.append((lambda kv, ref=ref: old_part(ref, kv), fade, None))
        for b, d in enumerate(which):
            low, high = half_refs[2 * b : 2 * b + 2]
            both = lambda kv, low=low, high=high: jnp.concatenate([new_part(low, kv), new_part(high, kv)], axis=0)
            chunks.append((both, None, spread(0, rows, d)))
        groups = [chunks[i : i + 2] for i in range(0, len(chunks), 2)]

        def score(r):
            q = q_refs[r][0, 0]
            row_pos = shard(r, 0) * rows + lax.broadcasted_iota(jnp.int32, (tile, DH), 0) % rows
            top = None
            for g, group in enumerate(groups):
                keys = jnp.concatenate([c[0](0) for c in group], axis=0)
                part = lax.dot_general(
                    q, keys, (((1,), (1,)), ((), ())), preferred_element_type=jnp.float32
                )
                for c, (_, fade, pos) in enumerate(group):
                    piece = part[:, c * DH : (c + 1) * DH]
                    if fade is not None:
                        piece = piece + fade
                    else:
                        piece = jnp.where(pos <= row_pos, piece, NEG)
                    score_ref[r % 2, 2 * g + c] = piece
                    top = piece if top is None else jnp.maximum(top, piece)
            return top

        def mix(r, top):
            at = slice(r * tile, (r + 1) * tile)
            top = jnp.broadcast_to(jnp.max(top, axis=-1, keepdims=True), (tile, DH))
            if state is not None:
                old_top = top_in[0, at, :]
                top = jnp.maximum(top, old_top)
            mixed = None
            for g, group in enumerate(groups):
                weights = [
                    jnp.exp2((score_ref[r % 2, 2 * g + c] - top) * SCALE).astype(jnp.bfloat16)
                    for c in range(len(group))
                ]
                values = jnp.concatenate([c[0](1) for c in group], axis=0)
                part = jnp.dot(
                    jnp.concatenate(weights, axis=1),
                    jnp.concatenate([values, jnp.ones_like(values)], axis=1),
                    preferred_element_type=jnp.float32,
                )
                mixed = part if mixed is None else mixed + part
            total, mixed = mixed[:, DH:], mixed[:, :DH]
            if state is not None:
                shrink = jnp.exp2((old_top - top) * SCALE)
                mixed = mixed + mixed_in[0, at, :DH] * shrink
                total = total + mixed_in[0, at, DH:] * shrink
            if last:
                rest[r][0] = (mixed / total).astype(jnp.bfloat16)
            else:
                rest[0][0, at, :DH] = mixed
                rest[0][0, at, DH:] = total
                rest[1][0, at, :] = top

        tops = score(0)
        for r in range(QUAD):
            following = score(r + 1) if r + 1 < QUAD else None
            mix(r, tops)
            tops = following

    half_shape = (slots, 2, 1, 1) + blocks[0][0].shape[4:]
    state_specs = [
        pl.BlockSpec((1, QUAD * tile, 2 * DH), lambda h: (h, 0, 0)),
        pl.BlockSpec((1, QUAD * tile, DH), lambda h: (h, 0, 0)),
    ]
    in_specs = [pl.BlockSpec(memory_space=pltpu.SMEM)] * 2
    in_specs += [pl.BlockSpec((1, 1, tile, DH), lambda h: (s, h, 0, 0))] * QUAD
    in_specs += [pl.BlockSpec(half_shape, lambda h: (0, 0, s, h, 0, 0))] * (2 * count)
    operands = [place, prefix_len, *queries, *[half for block in blocks for half in block]]
    if state is not None:
        in_specs += state_specs
        operands += list(state)
    if last:
        out_specs = [pl.BlockSpec((1, tile, DH), lambda h: (h, 0, 0))] * QUAD
        out_shape = [jax.ShapeDtypeStruct((KH, tile, DH), jnp.bfloat16)] * QUAD
    else:
        out_specs = state_specs
        out_shape = [jax.ShapeDtypeStruct((KH, QUAD * tile, w), jnp.float32) for w in (2 * DH, DH)]
    wide = count * (QUAD * (pre + rows)) // DH
    pairs = KH * QUAD * tile * wide * DH
    return pl.pallas_call(
        body,
        grid=(KH,),
        in_specs=in_specs,
        out_specs=out_specs,
        out_shape=out_shape,
        scratch_shapes=[pltpu.VMEM((2, wide, tile, DH), jnp.float32)],
        cost_estimate=pl.CostEstimate(flops=4 * DH * pairs, transcendentals=pairs, bytes_accessed=4 << 20),
        compiler_params=pltpu.CompilerParams(vmem_limit_bytes=ATTEND_VMEM),
        name="attend",
    )(*operands)


def send(array, perm):
    return lax.ppermute(array, "seq", perm)


def run(queries, stretch_keys, stretch_values, cache_keys, cache_values, prefix_len):
    seqs, rows, _ = queries.shape
    place = lax.axis_index("seq").astype(jnp.int32).reshape(1)

    pieces = pack_kv(place, cache_keys, cache_values, stretch_keys, stretch_values)
    got = [pieces[0]] + [send(pieces[r], quad_perm(r)) for r in range(1, QUAD)]
    packed = pack_q(place, queries)
    q_tiles = [packed[0]] + [send(packed[r], quad_perm(r)) for r in range(1, QUAD)]
    prefix_bounds, stretch_bounds = bounds(place, prefix_len, cache_keys, stretch_keys)

    rings = []
    for n in range(2):
        ring = {0: jnp.stack(got[2 * n : 2 * n + 2])}
        for step in range(1, RING // 2 + 1):
            if step < RING // 2 or n == 0:
                ring[-step % RING] = send(ring[(1 - step) % RING], ring_perm(1))
            if step < RING // 2 or n == 1:
                ring[step] = send(ring[step - 1], ring_perm(-1))
        rings.append(ring)

    sent = []
    for s in range(seqs):
        state = None
        for n, which in enumerate(PHASES):
            last = n + 1 == len(PHASES)
            blocks = [(rings[0][d], rings[1][d]) for d in which]
            state = attend(s, place, prefix_len, q_tiles, blocks, which, state, last, rows)
        sent.append([state[0]] + [send(state[r], quad_perm(r)) for r in range(1, QUAD)])
    attention = unpack_out(place, sent, rows)
    return attention, prefix_bounds, stretch_bounds


def solution(mesh):
    return jax.shard_map(
        run,
        mesh=mesh,
        in_specs=(
            P("grp", "seq", None),
            P("grp", "seq", None),
            P("grp", "seq", None),
            P("grp", "seq", None),
            P("grp", "seq", None),
            P("grp"),
        ),
        out_specs=(P("grp", "seq", None), P("grp", "seq", None), P("grp", "seq", None)),
        check_vma=False,
    )
```

```python
import math

import jax
import jax.numpy as jnp
from jax import lax
from jax.experimental import pallas as pl
from jax.experimental.pallas import tpu as pltpu
from jax.sharding import PartitionSpec as P


HQ = 64
HK = 8
DH = 128
PAGE = 16
GROUP = HQ // HK
NEG = -1e30
QUAD = 4
RING = 8
KH = HK // QUAD
ATTEND_VMEM = 24 << 20
SMALL_VMEM = 8 << 20
SCALE = math.log2(math.e) / math.sqrt(DH)


def ring_perm(step):
    return [(i, (i // 16) * 16 + ((i // 2 + step) % RING) * 2 + i % 2) for i in range(32)]


def quad_perm(r):
    return [(i, i ^ ((r >> 1) * 16) ^ (r & 1)) for i in range(32)]


def corner(place_ref):
    return (place_ref[0] // 16) * 2 + place_ref[0] % 2


def pack_kv(place, cache_keys, cache_values, stretch_keys, stretch_values):
    seqs, pre, _ = cache_keys.shape
    new = stretch_keys.shape[1]

    def body(place_ref, ck, cv, sk, sv, *outs):
        own = corner(place_ref)
        for r in range(QUAD):
            for h in range(KH):
                at = pl.ds(pl.multiple_of((own ^ r) * (KH * DH) + h * DH, DH), DH)
                for kv, (old, fresh) in enumerate(((ck, sk), (cv, sv))):
                    for s in range(seqs):
                        outs[r][kv, s, h, :pre, :] = old[s, :, at]
                        outs[r][kv, s, h, pre:, :] = fresh[s, :, at]

    shape = jax.ShapeDtypeStruct((2, seqs, KH, pre + new, DH), jnp.bfloat16)
    return pl.pallas_call(
        body,
        in_specs=[pl.BlockSpec(memory_space=pltpu.SMEM)] + [pl.BlockSpec(memory_space=pltpu.VMEM)] * 4,
        out_specs=[pl.BlockSpec(memory_space=pltpu.VMEM)] * QUAD,
        out_shape=[shape] * QUAD,
        compiler_params=pltpu.CompilerParams(vmem_limit_bytes=SMALL_VMEM),
        name="pack_kv",
    )(place, *[pltpu.with_memory_space_constraint(x, pltpu.HBM) for x in (cache_keys, cache_values, stretch_keys, stretch_values)])


def pack_q(place, queries):
    seqs, rows, _ = queries.shape

    def body(place_ref, q, *outs):
        own = corner(place_ref)
        for r in range(QUAD):
            for h in range(KH):
                for g in range(GROUP):
                    at = (own ^ r) * (KH * GROUP * DH) + (h * GROUP + g) * DH
                    outs[r][0, h, g * rows : (g + 1) * rows, :] = q[0, :, pl.ds(pl.multiple_of(at, DH), DH)]

    block = (1, KH, GROUP * rows, DH)
    return pl.pallas_call(
        body,
        grid=(seqs,),
        in_specs=[pl.BlockSpec(memory_space=pltpu.SMEM), pl.BlockSpec((1, rows, HQ * DH), lambda s: (s, 0, 0))],
        out_specs=[pl.BlockSpec(block, lambda s: (s, 0, 0, 0))] * QUAD,
        out_shape=[jax.ShapeDtypeStruct((seqs,) + block[1:], jnp.bfloat16)] * QUAD,
        compiler_params=pltpu.CompilerParams(vmem_limit_bytes=SMALL_VMEM),
        name="pack_q",
    )(place, queries)


def unpack_out(place, pieces, rows):
    seqs = len(pieces)

    def body(place_ref, *refs):
        own = corner(place_ref)
        out = refs[-1]
        for s in range(seqs):
            for r in range(QUAD):
                for h in range(KH):
                    for g in range(GROUP):
                        at = (own ^ r) * (KH * GROUP * DH) + (h * GROUP + g) * DH
                        piece = refs[s * QUAD + r][h, g * rows : (g + 1) * rows, :]
                        out[s, :, pl.ds(pl.multiple_of(at, DH), DH)] = piece

    return pl.pallas_call(
        body,
        in_specs=[pl.BlockSpec(memory_space=pltpu.SMEM)] + [pl.BlockSpec(memory_space=pltpu.VMEM)] * (seqs * QUAD),
        out_specs=pl.BlockSpec(memory_space=pltpu.VMEM),
        out_shape=jax.ShapeDtypeStruct((seqs, rows, HQ * DH), jnp.bfloat16),
        compiler_params=pltpu.CompilerParams(vmem_limit_bytes=SMALL_VMEM),
        name="unpack_out",
    )(place, *[p for one in pieces for p in one])


def bounds(place, prefix_len, cache_keys, stretch_keys):
    seqs, pre, width = cache_keys.shape
    new = stretch_keys.shape[1]

    def body(place_ref, len_ref, ck, sk, pre_out, new_out):
        first = place_ref[0] * (pre // PAGE)
        for s in range(seqs):
            for p in range(pre // PAGE):
                rows = ck[s, p * PAGE : (p + 1) * PAGE, :].astype(jnp.float32)
                live = (first + p) * PAGE < len_ref[s]
                low = jnp.where(live, jnp.min(rows, axis=0, keepdims=True), 0.0)
                high = jnp.where(live, jnp.max(rows, axis=0, keepdims=True), 0.0)
                pre_out[s, p : p + 1, :width] = low.astype(jnp.bfloat16)
                pre_out[s, p : p + 1, width:] = high.astype(jnp.bfloat16)
            for p in range(new // PAGE):
                rows = sk[s, p * PAGE : (p + 1) * PAGE, :].astype(jnp.float32)
                new_out[s, p : p + 1, :width] = jnp.min(rows, axis=0, keepdims=True).astype(jnp.bfloat16)
                new_out[s, p : p + 1, width:] = jnp.max(rows, axis=0, keepdims=True).astype(jnp.bfloat16)

    return pl.pallas_call(
        body,
        in_specs=[pl.BlockSpec(memory_space=pltpu.SMEM)] * 2 + [pl.BlockSpec(memory_space=pltpu.VMEM)] * 2,
        out_specs=[pl.BlockSpec(memory_space=pltpu.VMEM)] * 2,
        out_shape=[
            jax.ShapeDtypeStruct((seqs, pre // PAGE, 2 * width), jnp.bfloat16),
            jax.ShapeDtypeStruct((seqs, new // PAGE, 2 * width), jnp.bfloat16),
        ],
        compiler_params=pltpu.CompilerParams(vmem_limit_bytes=SMALL_VMEM),
        name="page_bounds",
    )(place, prefix_len, cache_keys, stretch_keys)


def attend(seqs, tiles, place, prefix_len, queries, parts, states, last, rows):
    tile = GROUP * rows
    arrays = [x for _, _, held in parts for x in held]
    pre = arrays[0].shape[4] - rows
    sources = []
    for d, slot, held in parts:
        for x in held:
            at = next(i for i, y in enumerate(arrays) if y is x)
            for i in range(x.shape[0]):
                sources.append((d, slot, at, i))
                slot += 1
    old_groups = [sources[i : i + DH // pre] for i in range(0, len(sources), DH // pre)]
    new_groups = [sources[i : i + DH // rows] for i in range(0, len(sources), DH // rows)]
    wide = len(old_groups) + len(new_groups)
    jobs = [(i, r) for i in range(len(seqs)) for r in range(len(tiles))]
    begun = states is not None

    def body(*refs):
        refs = list(refs)
        place_ref, len_ref, score_ref = refs.pop(0), refs.pop(0), refs.pop()
        take = lambda n: [refs.pop(0) for _ in range(n)]
        q_refs = {job: take(1)[0] for job in jobs}
        kv_refs = [take(len(arrays)) for _ in seqs]
        state_refs = [take(2) for _ in seqs] if begun else None
        out_refs = [take(len(tiles) if last else 2) for _ in seqs]
        own = corner(place_ref)
        z = (place_ref[0] // 2) % RING
        lane = lax.broadcasted_iota(jnp.int32, (1, DH), 1)

        def shard(slot, d):
            peer = own ^ slot
            return (peer // 2) * 16 + peer % 2 + ((z + d) % RING) * 2

        def spread(group, width):
            pos = shard(group[0][1], group[0][0]) * width + lane
            for k, (d, slot, _, _) in enumerate(group[1:], 1):
                pos = jnp.where(lane >= k * width, shard(slot, d) * width + lane - k * width, pos)
            return pos

        old_pos = [spread(group, pre) for group in old_groups]
        new_pos = [spread(group, rows) for group in new_groups]

        def rows_of(i, kv, c):
            if c < len(old_groups):
                group, at = old_groups[c], slice(0, pre)
            else:
                group, at = new_groups[c - len(old_groups)], slice(pre, pre + rows)
            return jnp.concatenate([kv_refs[i][x][k, kv, 0, 0, at, :] for _, _, x, k in group], axis=0)

        fades = [[jnp.where(pos < len_ref[s], 0.0, NEG) for pos in old_pos] for s in seqs]
        pairs = [range(c, min(c + 2, wide)) for c in range(0, wide, 2)]

        def positions(job):
            return shard(tiles[job[1]], 0) * rows + lax.broadcasted_iota(jnp.int32, (tile, DH), 0) % rows

        def score(n, pair, row_pos, top):
            i = jobs[n][0]
            keys = jnp.concatenate([rows_of(i, 0, c) for c in pair], axis=0)
            part = lax.dot_general(
                q_refs[jobs[n]][0, 0], keys, (((1,), (1,)), ((), ())), preferred_element_type=jnp.float32
            )
            for k, c in enumerate(pair):
                piece = part[:, k * DH : (k + 1) * DH]
                if c < len(old_groups):
                    piece = piece + fades[i][c]
                else:
                    piece = jnp.where(new_pos[c - len(old_groups)] <= row_pos, piece, NEG)
                score_ref[n % 2, c] = piece
                top = piece if top is None else jnp.maximum(top, piece)
            return top

        def settle(job, top):
            top = jnp.broadcast_to(jnp.max(top, axis=-1, keepdims=True), (tile, DH))
            if begun:
                top = jnp.maximum(top, state_refs[job[0]][1][0, job[1] * tile : (job[1] + 1) * tile, :])
            return top

        def mix(n, pair, top, mixed):
            weights = [jnp.exp2((score_ref[n % 2, c] - top) * SCALE).astype(jnp.bfloat16) for c in pair]
            values = jnp.concatenate([rows_of(jobs[n][0], 1, c) for c in pair], axis=0)
            part = jnp.dot(
                jnp.concatenate(weights, axis=1),
                jnp.concatenate([values, jnp.ones_like(values)], axis=1),
                preferred_element_type=jnp.float32,
            )
            return part if mixed is None else mixed + part

        def finish(job, top, mixed):
            i, r = job
            at = slice(r * tile, (r + 1) * tile)
            total, mixed = mixed[:, DH:], mixed[:, :DH]
            if begun:
                mixed_in, top_in = state_refs[i]
                shrink = jnp.exp2((top_in[0, at, :] - top) * SCALE)
                mixed = mixed + mixed_in[0, at, :DH] * shrink
                total = total + mixed_in[0, at, DH:] * shrink
            if last:
                out_refs[i][r][0] = (mixed / total).astype(jnp.bfloat16)
            else:
                out_refs[i][0][0, at, :DH] = mixed
                out_refs[i][0][0, at, DH:] = total
                out_refs[i][1][0, at, :] = top

        top = None
        for pair in pairs:
            top = score(0, pair, positions(jobs[0]), top)
        for n, job in enumerate(jobs):
            top = settle(job, top)
            following, mixed = None, None
            for pair in pairs:
                if n + 1 < len(jobs):
                    following = score(n + 1, pair, positions(jobs[n + 1]), following)
                mixed = mix(n, pair, top, mixed)
            finish(job, top, mixed)
            top = following

    part = tiles[0] // len(tiles)
    state_specs = [
        pl.BlockSpec((1, len(tiles) * tile, 2 * DH), lambda h: (h, part, 0)),
        pl.BlockSpec((1, len(tiles) * tile, DH), lambda h: (h, part, 0)),
    ]
    in_specs = [pl.BlockSpec(memory_space=pltpu.SMEM)] * 2
    operands = [place, prefix_len]
    for i, r in jobs:
        in_specs.append(pl.BlockSpec((1, 1, tile, DH), lambda h, s=seqs[i]: (s, h, 0, 0)))
        operands.append(queries[tiles[r]])
    for s in seqs:
        in_specs += [
            pl.BlockSpec(x.shape[:2] + (1, 1) + x.shape[4:], lambda h, s=s: (0, 0, s, h, 0, 0)) for x in arrays
        ]
        operands += arrays
    if begun:
        in_specs += state_specs * len(seqs)
        operands += [x for s in seqs for x in states[s]]
    if last:
        out_specs = [pl.BlockSpec((1, tile, DH), lambda h: (h, 0, 0))] * len(jobs)
        out_shape = [jax.ShapeDtypeStruct((KH, tile, DH), jnp.bfloat16)] * len(jobs)
    else:
        out_specs = state_specs * len(seqs)
        out_shape = [jax.ShapeDtypeStruct((KH, QUAD * tile, w), jnp.float32) for w in (2 * DH, DH)] * len(seqs)
    count = KH * len(jobs) * tile * wide * DH
    outs = pl.pallas_call(
        body,
        grid=(KH,),
        in_specs=in_specs,
        out_specs=out_specs,
        out_shape=out_shape,
        scratch_shapes=[pltpu.VMEM((2, wide, tile, DH), jnp.float32)],
        cost_estimate=pl.CostEstimate(flops=4 * DH * count, transcendentals=count, bytes_accessed=4 << 20),
        compiler_params=pltpu.CompilerParams(vmem_limit_bytes=ATTEND_VMEM),
        name="attend",
    )(*operands)
    each = len(outs) // len(seqs)
    return {s: outs[i * each : (i + 1) * each] for i, s in enumerate(seqs)}


def send(array, perm):
    return lax.ppermute(array, "seq", perm)


def run(queries, stretch_keys, stretch_values, cache_keys, cache_values, prefix_len):
    seqs, rows, _ = queries.shape
    place = lax.axis_index("seq").astype(jnp.int32).reshape(1)

    pieces = pack_kv(place, cache_keys, cache_values, stretch_keys, stretch_values)
    got = [pieces[0]] + [send(pieces[r], quad_perm(r)) for r in range(1, QUAD)]
    packed = pack_q(place, queries)
    q_tiles = [packed[0]] + [send(packed[r], quad_perm(r)) for r in range(1, QUAD)]
    prefix_bounds, stretch_bounds = bounds(place, prefix_len, cache_keys, stretch_keys)

    half = RING // 2
    rings = []
    for n in range(2):
        ring = {0: [jnp.stack(got[2 * n : 2 * n + 2])]}
        for step in range(1, half):
            ring[-step % RING] = [send(ring[(1 - step) % RING][0], ring_perm(1))]
            ring[step] = [send(ring[step - 1][0], ring_perm(-1))]
        rings.append(ring)
    for n in range(2):
        rings[n][half] = [send(rings[n][half + 1][0][:1], ring_perm(1)), send(rings[n][half - 1][0][1:], ring_perm(-1))]

    whole = lambda *ds: [(d, 0, rings[0][d] + rings[1][d]) for d in ds]
    common = (place, prefix_len, q_tiles)
    every = tuple(range(QUAD))
    states = {}
    for s in range(seqs):
        states.update(attend((s,), every, *common, whole(0, 7, 1), None, False, rows))
    states = attend((0, 1), every, *common, whole(6, 2), states, False, rows)
    for n in range(2):
        held = [(d, 2 * n, rings[n][d]) for d in (5, 3)]
        states = attend((0, 1), every, *common, held, states, False, rows)

    sent = [[None] * QUAD for _ in range(seqs)]
    for group, tiles in (((1,), (2, 3)), ((0,), (2, 3)), ((0, 1), (0, 1))):
        done = attend(group, tiles, *common, whole(half), states, True, rows)
        for s in group:
            for r, out in zip(tiles, done[s]):
                sent[s][r] = send(out, quad_perm(r)) if r else out
    attention = unpack_out(place, sent, rows)
    return attention, prefix_bounds, stretch_bounds


def solution(mesh):
    return jax.shard_map(
        run,
        mesh=mesh,
        in_specs=(
            P("grp", "seq", None),
            P("grp", "seq", None),
            P("grp", "seq", None),
            P("grp", "seq", None),
            P("grp", "seq", None),
            P("grp"),
        ),
        out_specs=(P("grp", "seq", None), P("grp", "seq", None), P("grp", "seq", None)),
        check_vma=False,
    )
```
